32 devices in a mesh: tp: 4 (over z), dp: 8 (over y, x, core).
Axes of the slice: x: 2, y: 2, z: 4, core: 2. Of those that a mesh axis runs over, the one named last changes fastest.
Arguments:
- hidden: bfloat16 [32, 512, 5120], P('dp')
- gain_in: float32 [5120], replicated
- gain_q: float32 [1536], replicated
- gain_kv: float32 [512], replicated
- w_qa: bfloat16 [5120, 1536], replicated
- w_kva: bfloat16 [5120, 576], replicated
- w_qb: bfloat16 [1536, 24576], P(None, 'tp')
- w_kvb: bfloat16 [512, 32768], P(None, 'tp')
- w_out: bfloat16 [16384, 5120], P('tp')
Outputs:
- output 1: bfloat16 [32, 512, 5120], P('dp')
- output 2: float32 [128], replicated
- output 3: bfloat16 [1536, 24576], P(None, 'tp')
- output 4: bfloat16 [512, 32768], P(None, 'tp')
All inputs are finite; a program needn't handle non-finite values.
Results may differ from the reference program's by a relative error of at most 0.00727548.
Values sent between devices are 32-bit elements.
A program may use at most 1 GiB of HBM per device.

```python
import math
import jax
import jax.numpy as jnp
from jax import lax

B_ALL = 32
SEQ_LEN = 512
D = 5120
HEADS = 128
Q_LORA = 1536
KV_LORA = 512
NOPE_DIM = 128
ROPE_DIM = 64
V_DIM = 128
CLIP_TAU = 100

QK_DIM = NOPE_DIM + ROPE_DIM
NORM_EPS = 1e-6
ROPE_BASE = 50000.0
MSCALE_SQ = (0.1 * math.log(32.0) + 1.0) ** 2
LOGIT_SCALE = QK_DIM ** -0.5 * MSCALE_SQ


def rms_norm(tensor, gain_vec):
    return tensor * lax.rsqrt(jnp.mean(tensor * tensor, axis=-1, keepdims=True) + NORM_EPS) * gain_vec


def rotate(tensor, cos_table, sin_table):
    half_dim = ROPE_DIM // 2
    first_half = tensor[..., :half_dim]
    second_half = tensor[..., half_dim:]
    return jnp.concatenate([first_half * cos_table - second_half * sin_table, first_half * sin_table + second_half * cos_table], axis=-1)


def column_gains(first_gain, first_dim, second_gain, second_dim):
    return jnp.concatenate([jnp.broadcast_to(first_gain[:, None], (HEADS, first_dim)), jnp.broadcast_to(second_gain[:, None], (HEADS, second_dim))], axis=1).reshape(-1)


def setup_inputs(seed: int = 0) -> dict:
    key_list = jax.random.split(jax.random.key(seed), 14)
    common = jax.random.normal(key_list[0], (B_ALL, 1, D), jnp.float32)
    noise_part = jax.random.normal(key_list[1], (B_ALL, SEQ_LEN, D), jnp.float32)
    free_draw = jax.random.randint(key_list[2], (B_ALL,), 0, 64)
    free_pick = jax.random.randint(key_list[3], (), 0, B_ALL)
    independent = (free_draw == 0) | (jnp.arange(B_ALL) == free_pick)
    share_w = jnp.where(independent, 0.0, 0.9)[:, None, None]
    hidden = (share_w * common + jnp.sqrt(1.0 - share_w * share_w) * noise_part).astype(jnp.bfloat16)
    gain_in = 1.0 + 0.2 * jax.random.normal(key_list[4], (D,), jnp.float32)
    gain_q = 1.0 + 0.2 * jax.random.normal(key_list[5], (Q_LORA,), jnp.float32)
    gain_kv = 1.0 + 0.2 * jax.random.normal(key_list[6], (KV_LORA,), jnp.float32)
    w_qa = (jax.random.normal(key_list[7], (D, Q_LORA), jnp.float32) * D ** -0.5).astype(jnp.bfloat16)
    w_kva = (jax.random.normal(key_list[8], (D, KV_LORA + ROPE_DIM), jnp.float32) * D ** -0.5).astype(jnp.bfloat16)
    target = CLIP_TAU / (MSCALE_SQ * math.sqrt(2.0 * math.log(0.5 * SEQ_LEN * SEQ_LEN)))
    head_scale = jnp.exp(jax.random.uniform(key_list[9], (HEADS,), jnp.float32, math.log(0.5), math.log(2.5))) * target
    w_qb = (jax.random.normal(key_list[10], (Q_LORA, HEADS, QK_DIM), jnp.float32) * head_scale[None, :, None] * Q_LORA ** -0.5).reshape(Q_LORA, HEADS * QK_DIM).astype(jnp.bfloat16)
    w_kvb = (jax.random.normal(key_list[11], (KV_LORA, HEADS * (NOPE_DIM + V_DIM)), jnp.float32) * KV_LORA ** -0.5).astype(jnp.bfloat16)
    w_out = (jax.random.normal(key_list[12], (HEADS * V_DIM, D), jnp.float32) * (HEADS * V_DIM) ** -0.5).astype(jnp.bfloat16)
    return {'hidden': hidden, 'gain_in': gain_in, 'gain_q': gain_q, 'gain_kv': gain_kv, 'w_qa': w_qa, 'w_kva': w_kva, 'w_qb': w_qb, 'w_kvb': w_kvb, 'w_out': w_out}


def reference(hidden, gain_in, gain_q, gain_kv, w_qa, w_kva, w_qb, w_kvb, w_out):
    positions = jnp.arange(SEQ_LEN, dtype=jnp.float32)
    inv_freq = ROPE_BASE ** (-2.0 * jnp.arange(ROPE_DIM // 2, dtype=jnp.float32) / ROPE_DIM)
    angles = positions[:, None] * inv_freq[None, :]
    cos_table = jnp.cos(angles)
    sin_table = jnp.sin(angles)
    causal = jnp.arange(SEQ_LEN)[:, None] >= jnp.arange(SEQ_LEN)[None, :]

    def per_sequence(tokens):
        normed = rms_norm(tokens.astype(jnp.float32), gain_in).astype(jnp.bfloat16)
        q_lat = rms_norm(jnp.dot(normed, w_qa, preferred_element_type=jnp.float32), gain_q).astype(jnp.bfloat16)
        kv_lat = jnp.dot(normed, w_kva, preferred_element_type=jnp.float32)
        latent = rms_norm(kv_lat[:, :KV_LORA], gain_kv).astype(jnp.bfloat16)
        k_rot = rotate(kv_lat[:, KV_LORA:], cos_table, sin_table).astype(jnp.bfloat16)
        q_full = jnp.dot(q_lat, w_qb, preferred_element_type=jnp.float32).reshape(SEQ_LEN, HEADS, QK_DIM)
        q_nope = q_full[..., :NOPE_DIM].astype(jnp.bfloat16)
        q_rot = rotate(q_full[..., NOPE_DIM:], cos_table[:, None, :], sin_table[:, None, :]).astype(jnp.bfloat16)
        kv_full = jnp.dot(latent, w_kvb, preferred_element_type=jnp.float32).astype(jnp.bfloat16).reshape(SEQ_LEN, HEADS, NOPE_DIM + V_DIM)
        k_nope = kv_full[..., :NOPE_DIM].astype(jnp.float32)
        values = kv_full[..., NOPE_DIM:].astype(jnp.float32)
        logits = jnp.einsum('qhd,khd->hqk', q_nope.astype(jnp.float32), k_nope) + jnp.einsum('qhd,kd->hqk', q_rot.astype(jnp.float32), k_rot.astype(jnp.float32))
        logits = jnp.where(causal[None], logits * LOGIT_SCALE, -jnp.inf)
        attn_prob = jax.nn.softmax(logits, axis=-1).astype(jnp.bfloat16)
        attn_out = jnp.einsum('hqk,khd->qhd', attn_prob.astype(jnp.float32), values).astype(jnp.bfloat16).reshape(SEQ_LEN, HEADS * V_DIM)
        update = jnp.dot(attn_out, w_out, preferred_element_type=jnp.float32)
        return (tokens.astype(jnp.float32) + update).astype(jnp.bfloat16), jnp.max(logits, axis=(1, 2))

    out_hidden, seq_max = lax.map(per_sequence, hidden)
    logit_max = jnp.max(seq_max, axis=0)
    clip_gain = CLIP_TAU / jnp.maximum(CLIP_TAU, logit_max)
    root_gain = jnp.sqrt(clip_gain)
    new_qb = (w_qb.astype(jnp.float32) * column_gains(root_gain, NOPE_DIM, clip_gain, ROPE_DIM)[None, :]).astype(jnp.bfloat16)
    new_kvb = (w_kvb.astype(jnp.float32) * column_gains(root_gain, NOPE_DIM, jnp.ones_like(clip_gain), V_DIM)[None, :]).astype(jnp.bfloat16)
    return out_hidden, logit_max, new_qb, new_kvb
```

```python
import math
import jax
import jax.numpy as jnp
from jax import lax
from jax.experimental import pallas as pl
from jax.experimental.pallas import tpu as pltpu
from jax.sharding import PartitionSpec as P

NORM_EPS = 1e-6
ROPE_BASE = 50000.0
MSCALE_SQ = (0.1 * math.log(32.0) + 1.0) ** 2
CLIP_TAU = 100.0
MESH = pl.DeviceIdType.MESH
F32 = jnp.float32
BF16 = jnp.bfloat16

TILE = 256
DEPTH = 512
LAG_PAIR, LAG_MID, LAG_END = 2, 4, 6
SLOTS_P, SLOTS_1, SLOTS_2, SLOTS_3, SLOTS_T = 5, 7, 6, 7, 3


def rope_tables(seq_len, rope_dim):
    inv_freq = ROPE_BASE ** (-2.0 * jnp.arange(rope_dim // 2, dtype=F32) / rope_dim)
    angles = jnp.arange(seq_len).astype(F32)[:, None] * inv_freq[None, :]
    cos, sin = jnp.cos(angles), jnp.sin(angles)
    blank = jnp.zeros((seq_len, 128 - rope_dim), F32)
    return jnp.concatenate([cos, cos, blank], axis=1), jnp.concatenate([-sin, sin, blank], axis=1)


def column_gains(first_gain, first_dim, second_gain, second_dim):
    num_heads = first_gain.shape[0]
    return jnp.concatenate([jnp.broadcast_to(first_gain[:, None], (num_heads, first_dim)), jnp.broadcast_to(second_gain[:, None], (num_heads, second_dim))], axis=1).reshape(-1)


def rescale(weight, col_gain):
    return (weight.astype(F32) * col_gain[None, :]).astype(BF16)


def dot(a, b):
    return jnp.dot(a, b, preferred_element_type=F32)


def kernel(dims, x_hbm, gin, gq, gkv, cos, sin, wqa_hbm, wkva_hbm, wqb_hbm, wkvb_hbm, wout_hbm,
           y_hbm, gall, gmine,
           xn, accq, acck, cq, ckv, krot, obuf, wqa, wkva, wqb, wkvb, wout,
           pbuf, r1, r2, r3, tbuf, xt, yt, smax, srecv,
           x_sem, a_sem, b_sem, o_sem, xt_sem, yt_sem,
           p_send, r1_recv, a_send, r2_recv, t_send, r3_recv, st_send, st_recv, g_send, g_recv):
    num_seqs, seq_len, model_dim, scale, rope_dim = dims
    q_rank = cq.shape[1]
    kv_rank = ckv.shape[1]
    tiles = model_dim // TILE
    units = model_dim // DEPTH
    pairs = wqb_hbm.shape[1] // 384
    total = num_seqs * tiles
    z = lax.axis_index("tp")
    dp = lax.axis_index("dp")
    is_mid = jnp.logical_or(z == 1, z == 2)
    is_end = jnp.logical_or(z == 0, z == 3)
    near = z + 1 - 2 * (z % 2)
    across = 3 - z
    dp_peer = [dp + 1 - 2 * (dp % 2), dp + 2 - 4 * ((dp // 2) % 2), dp + 4 - 8 * (dp // 4)]
    tp_peer = [(z + d) % 4 for d in (1, 2, 3)]

    barrier = pltpu.get_barrier_semaphore()
    for peer in dp_peer:
        pl.semaphore_signal(barrier, inc=1, device_id={"dp": peer}, device_id_type=MESH)
    for peer in tp_peer:
        pl.semaphore_signal(barrier, inc=1, device_id={"tp": peer}, device_id_type=MESH)
    pl.semaphore_wait(barrier, 6)

    def x_copy(seq):
        return pltpu.make_async_copy(x_hbm.at[seq], xn, x_sem)

    def a_copies(u):
        slot = u % 2
        rows = pl.ds(pl.multiple_of(u * DEPTH, DEPTH), DEPTH)
        return (pltpu.make_async_copy(wqa_hbm.at[rows], wqa.at[slot], a_sem.at[0, slot]),
                pltpu.make_async_copy(wkva_hbm.at[rows], wkva.at[slot], a_sem.at[1, slot]))

    def b_copies(hp):
        slot = hp % 2
        return (pltpu.make_async_copy(wqb_hbm.at[:, pl.ds(pl.multiple_of(hp * 384, 384), 384)], wqb.at[slot], b_sem.at[0, slot]),
                pltpu.make_async_copy(wkvb_hbm.at[:, pl.ds(pl.multiple_of(hp * 512, 512), 512)], wkvb.at[slot], b_sem.at[1, slot]))

    def cols_of(k):
        return pl.ds(pl.multiple_of((k % tiles) * TILE, TILE), TILE)

    def o_copy(k):
        return pltpu.make_async_copy(wout_hbm.at[:, cols_of(k)], wout.at[k % 2], o_sem.at[k % 2])

    def xt_copy(k):
        return pltpu.make_async_copy(x_hbm.at[k // tiles, :, cols_of(k)], xt, xt_sem)

    def yt_copy(k):
        return pltpu.make_async_copy(yt.at[k % 2], y_hbm.at[k // tiles, :, cols_of(k)], yt_sem.at[k % 2])

    def p_copy(k):
        return pltpu.make_async_remote_copy(
            src_ref=pbuf.at[k % SLOTS_P], dst_ref=r1.at[k % SLOTS_1], send_sem=p_send.at[k % SLOTS_P],
            recv_sem=r1_recv.at[k % SLOTS_1], device_id={"tp": near}, device_id_type=MESH)

    def a_copy(k):
        return pltpu.make_async_remote_copy(
            src_ref=pbuf.at[k % SLOTS_P], dst_ref=r2.at[k % SLOTS_2], send_sem=a_send.at[k % SLOTS_P],
            recv_sem=r2_recv.at[k % SLOTS_2], device_id={"tp": across}, device_id_type=MESH)

    def t_copy(k):
        return pltpu.make_async_remote_copy(
            src_ref=tbuf.at[k % SLOTS_T], dst_ref=r3.at[k % SLOTS_3], send_sem=t_send.at[k % SLOTS_T],
            recv_sem=r3_recv.at[k % SLOTS_3], device_id={"tp": near}, device_id_type=MESH)

    def st_copy(r):
        return pltpu.make_async_remote_copy(
            src_ref=smax, dst_ref=srecv.at[r], send_sem=st_send.at[r],
            recv_sem=st_recv.at[r], device_id={"dp": dp_peer[r]}, device_id_type=MESH)

    def g_copy(d):
        return pltpu.make_async_remote_copy(
            src_ref=smax, dst_ref=gall.at[z], send_sem=g_send.at[d],
            recv_sem=g_recv.at[d], device_id={"tp": tp_peer[d]}, device_id_type=MESH)

    def normalize():
        def block(i, carry):
            rows = pl.ds(pl.multiple_of(i * 16, 16), 16)
            v = xn[rows, :].astype(F32)
            inv = lax.rsqrt(jnp.mean(v * v, axis=-1, keepdims=True) + NORM_EPS)
            xn[rows, :] = (v * inv * gin[...]).astype(BF16)
            return carry
        lax.fori_loop(0, seq_len // 16, block, 0)

    def a_step(u):
        for c in a_copies(u):
            c.wait()

        @pl.when(u + 1 < units)
        def _():
            for c in a_copies(u + 1):
                c.start()

        slot = u % 2
        cols = pl.ds(pl.multiple_of(u * DEPTH, DEPTH), DEPTH)
        piece = xn[:, cols]
        width = 512

        @pl.when(u == 0)
        def _():
            for j in range(q_rank // width):
                accq[:, j * width:(j + 1) * width] = dot(piece, wqa[slot, :, j * width:(j + 1) * width])
            acck[...] = dot(piece, wkva[slot])

        @pl.when(u > 0)
        def _():
            for j in range(q_rank // width):
                accq[:, j * width:(j + 1) * width] += dot(piece, wqa[slot, :, j * width:(j + 1) * width])
            acck[...] += dot(piece, wkva[slot])

    def rope(v, c, s):
        half = rope_dim // 2
        lane = lax.broadcasted_iota(jnp.int32, v.shape, 1)
        swap = jnp.where(lane < half, pltpu.roll(v, 128 - half, 1), pltpu.roll(v, half, 1))
        return v * c + swap * s

    def finish_latents():
        def block(i, carry):
            rows = pl.ds(pl.multiple_of(i * 64, 64), 64)
            v = accq[rows, :]
            inv = lax.rsqrt(jnp.mean(v * v, axis=-1, keepdims=True) + NORM_EPS)
            cq[rows, :] = (v * inv * gq[...]).astype(BF16)
            w = acck[rows, :kv_rank]
            inv = lax.rsqrt(jnp.mean(w * w, axis=-1, keepdims=True) + NORM_EPS)
            ckv[rows, :] = (w * inv * gkv[...]).astype(BF16)
            kr = jnp.concatenate([acck[rows, kv_rank:], jnp.zeros((64, 128 - rope_dim), F32)], axis=1)
            krot[rows, :] = rope(kr, cos[rows, :], sin[rows, :]).astype(BF16)
            return carry
        lax.fori_loop(0, seq_len // 64, block, 0)

    def b_step(hp, oslot):
        for c in b_copies(hp):
            c.wait()

        @pl.when(hp + 1 < pairs)
        def _():
            for c in b_copies(hp + 1):
                c.start()

        slot = hp % 2
        qf = dot(cq[...], wqb[slot])
        kv = dot(ckv[...], wkvb[slot]).astype(BF16)
        qs = pltpu.roll(qf, 192, 1)
        blk = 256
        for head, q2 in ((0, qf), (1, qs)):
            q_rot = rope(q2[:, 128:256], cos[...], sin[...])
            qcat = jnp.concatenate([q2[:, :128].astype(BF16), q_rot.astype(BF16)], axis=1)
            kcat = jnp.concatenate([kv[:, head * 256:head * 256 + 128], krot[...]], axis=1)
            vals = kv[:, head * 256 + 128:head * 256 + 256]
            best = None
            for i in range(seq_len // blk):
                width = (i + 1) * blk
                l = lax.dot_general(qcat[i * blk:width], kcat[:width], (((1,), (1,)), ((), ())), preferred_element_type=F32) * scale
                row = lax.broadcasted_iota(jnp.int32, l.shape, 0) + i * blk
                col = lax.broadcasted_iota(jnp.int32, l.shape, 1)
                l = jnp.where(col <= row, l, -jnp.inf)
                m = jnp.max(l, axis=-1, keepdims=True)
                e = jnp.exp(l - m)
                p = (e * (1.0 / jnp.sum(e, axis=-1, keepdims=True))).astype(BF16)
                o = dot(p, vals[:width]).astype(BF16)
                obuf[oslot, i * blk:width, pl.ds(pl.multiple_of(hp * 256 + head * 128, 128), 128)] = o
                top = jnp.max(m, axis=0, keepdims=True)
                best = top if best is None else jnp.maximum(best, top)
            r = pl.ds(hp * 2 + head, 1)
            smax[r, :] = jnp.maximum(smax[r, :], jnp.broadcast_to(best, (1, 128)))

    def finish_tile(k, value):
        xt_copy(k).wait()

        @pl.when(k >= 2)
        def _():
            yt_copy(k - 2).wait()

        yt[k % 2] = (xt[...].astype(F32) + value).astype(BF16)
        yt_copy(k).start()

    smax[...] = jnp.full(smax.shape, -jnp.inf, F32)

    def tick(i):
        seq = i // tiles
        t = i % tiles
        tau = i - tiles

        done_tile = jnp.where(is_mid, tau - LAG_MID, tau - LAG_END)

        @pl.when(jnp.logical_and(done_tile >= 0, done_tile < total))
        def _():
            xt_copy(done_tile).start()

        @pl.when(i == 0)
        def _():
            o_copy(0).start()

        @pl.when(jnp.logical_and(is_end, jnp.logical_and(tau >= SLOTS_P, tau < total + SLOTS_P)))
        def _():
            p_copy(tau - SLOTS_P).wait_send()

        @pl.when(jnp.logical_and(tau >= 0, tau < total))
        def _():
            o_copy(tau).wait()

            @pl.when(tau + 1 < total)
            def _():
                o_copy(tau + 1).start()

            pbuf[tau % SLOTS_P] = dot(obuf[(tau // tiles) % 2], wout[tau % 2])

            @pl.when(is_end)
            def _():
                p_copy(tau).start()

        @pl.when(jnp.logical_and(is_mid, jnp.logical_and(tau >= LAG_PAIR, tau < total + LAG_PAIR)))
        def _():
            k = tau - LAG_PAIR
            p_copy(k).wait_recv()
            pbuf[k % SLOTS_P] = pbuf[k % SLOTS_P] + r1[k % SLOTS_1]
            a_copy(k).start()

        @pl.when(jnp.logical_and(is_mid, jnp.logical_and(tau >= LAG_MID, tau < total + LAG_MID)))
        def _():
            k = tau - LAG_MID
            a_copy(k).wait()

            @pl.when(k >= SLOTS_T)
            def _():
                t_copy(k - SLOTS_T).wait_send()

            value = pbuf[k % SLOTS_P] + r2[k % SLOTS_2]
            tbuf[k % SLOTS_T] = value
            t_copy(k).start()
            finish_tile(k, value)

        @pl.when(jnp.logical_and(is_end, jnp.logical_and(tau >= LAG_END, tau < total + LAG_END)))
        def _():
            k = tau - LAG_END
            t_copy(k).wait_recv()
            finish_tile(k, r3[k % SLOTS_3])

        @pl.when(seq < num_seqs)
        def _():
            @pl.when(t == 0)
            def _():
                x_copy(seq).start()
                for c in a_copies(0):
                    c.start()
                for c in b_copies(0):
                    c.start()
                x_copy(seq).wait()
                normalize()

            @pl.when(t < units // 2)
            def _():
                def two(j, carry):
                    a_step(2 * t + j)
                    return carry
                lax.fori_loop(0, 2, two, 0)

            @pl.when(t == units // 2 - 1)
            def _():
                finish_latents()

            @pl.when(t >= tiles - pairs)
            def _():
                b_step(t - (tiles - pairs), seq % 2)

    def stats_round(i):
        first = num_seqs * tiles
        for r in range(4):
            @pl.when(i == first + r)
            def _(r=r):
                if r > 0:
                    st_copy(r - 1).wait()
                    smax[...] = jnp.maximum(smax[...], srecv[r - 1])
                if r < 3:
                    st_copy(r).start()
                else:
                    gmine[...] = smax[...]
                    gall[z] = smax[...]
                    for d in range(3):
                        g_copy(d).start()

        @pl.when(i == first + 6)
        def _():
            for d in range(3):
                g_copy(d).wait()

    def whole_tick(i, carry):
        tick(i)
        stats_round(i)
        return carry

    lax.fori_loop(0, tiles + total + 7, whole_tick, 0)

    @pl.when(is_mid)
    def _():
        for k in range(total - SLOTS_T, total):
            t_copy(k).wait_send()
    for k in range(total - 2, total):
        yt_copy(k).wait()


def solution(mesh):
    def device_step(hidden, gain_in, gain_q, gain_kv, w_qa, w_kva, w_qb, w_kvb, w_out):
        num_seqs, seq_len, model_dim = hidden.shape
        q_rank, kv_rank = gain_q.shape[0], gain_kv.shape[0]
        rope_dim = w_kva.shape[1] - kv_rank
        num_heads = (w_qb.shape[1] - w_kvb.shape[1] + w_out.shape[0]) // rope_dim
        value_dim = w_out.shape[0] // num_heads
        nope_dim = w_kvb.shape[1] // num_heads - value_dim
        scale = (nope_dim + rope_dim) ** -0.5 * MSCALE_SQ
        cos, sin = rope_tables(seq_len, rope_dim)
        any_spec = pl.BlockSpec(memory_space=pl.ANY)
        vmem = pl.BlockSpec(memory_space=pltpu.VMEM)
        dma = pltpu.SemaphoreType.DMA
        block = (seq_len, TILE)
        y, gall, gmine = pl.pallas_call(
            lambda *refs: kernel((num_seqs, seq_len, model_dim, scale, rope_dim), *refs),
            out_shape=(jax.ShapeDtypeStruct(hidden.shape, BF16), jax.ShapeDtypeStruct((4, num_heads, 128), F32), jax.ShapeDtypeStruct((num_heads, 128), F32)),
            in_specs=[any_spec] + [vmem] * 5 + [any_spec] * 5,
            out_specs=(any_spec, vmem, vmem),
            scratch_shapes=[
                pltpu.VMEM((seq_len, model_dim), BF16),
                pltpu.VMEM((seq_len, q_rank), F32),
                pltpu.VMEM((seq_len, w_kva.shape[1]), F32),
                pltpu.VMEM((seq_len, q_rank), BF16),
                pltpu.VMEM((seq_len, kv_rank), BF16),
                pltpu.VMEM((seq_len, 128), BF16),
                pltpu.VMEM((2, seq_len, w_out.shape[0]), BF16),
                pltpu.VMEM((2, DEPTH, q_rank), BF16),
                pltpu.VMEM((2, DEPTH, w_kva.shape[1]), BF16),
                pltpu.VMEM((2, q_rank, 384), BF16),
                pltpu.VMEM((2, kv_rank, 512), BF16),
                pltpu.VMEM((2, w_out.shape[0], TILE), BF16),
                pltpu.VMEM((SLOTS_P,) + block, F32),
                pltpu.VMEM((SLOTS_1,) + block, F32),
                pltpu.VMEM((SLOTS_2,) + block, F32),
                pltpu.VMEM((SLOTS_3,) + block, F32),
                pltpu.VMEM((SLOTS_T,) + block, F32),
                pltpu.VMEM(block, BF16),
                pltpu.VMEM((2,) + block, BF16),
                pltpu.VMEM((num_heads, 128), F32),
                pltpu.VMEM((3, num_heads, 128), F32),
                dma, dma((2, 2)), dma((2, 2)), dma((2,)), dma, dma((2,)),
                dma((SLOTS_P,)), dma((SLOTS_1,)), dma((SLOTS_P,)), dma((SLOTS_2,)), dma((SLOTS_T,)), dma((SLOTS_3,)),
                dma((3,)), dma((3,)), dma((3,)), dma((3,)),
            ],
            compiler_params=pltpu.CompilerParams(collective_id=0, has_side_effects=True, vmem_limit_bytes=66 * 1000 * 1000),
            name="latent_attention",
        )(hidden, gain_in[None], gain_q[None], gain_kv[None], cos, sin, w_qa, w_kva, w_qb, w_kvb, w_out)
        head_max = gmine[:, 0]
        clip_gain = CLIP_TAU / jnp.maximum(CLIP_TAU, head_max)
        root_gain = jnp.sqrt(clip_gain)
        new_qb = rescale(w_qb, column_gains(root_gain, nope_dim, clip_gain, rope_dim))
        new_kvb = rescale(w_kvb, column_gains(root_gain, nope_dim, jnp.ones_like(clip_gain), value_dim))
        return y, gall[:, :, 0].reshape(-1), new_qb, new_kvb

    weight_spec = P(None, 'tp')
    return jax.shard_map(device_step, mesh=mesh, in_specs=(P('dp', None, None), P(), P(), P(), P(), P(), weight_spec, weight_spec, P('tp', None)), out_specs=(P('dp', None, None), P(), weight_spec, weight_spec), check_vma=False)
```

```python
import math
import jax
import jax.numpy as jnp
from jax import lax
from jax.experimental import pallas as pl
from jax.experimental.pallas import tpu as pltpu
from jax.sharding import PartitionSpec as P

NORM_EPS = 1e-6
ROPE_BASE = 50000.0
MSCALE_SQ = (0.1 * math.log(32.0) + 1.0) ** 2
CLIP_TAU = 100.0
MESH = pl.DeviceIdType.MESH
F32 = jnp.float32
BF16 = jnp.bfloat16

ROWS = 256
TILE = 512
DEPTH = 512
A_TICKS = 2
LAG_PAIR, LAG_MID, LAG_END = 2, 4, 6
SLOTS_P, SLOTS_1, SLOTS_2, SLOTS_3, SLOTS_T = 5, 7, 6, 7, 3


def rope_tables(seq_len, rope_dim):
    inv_freq = ROPE_BASE ** (-2.0 * jnp.arange(rope_dim // 2, dtype=F32) / rope_dim)
    angles = jnp.arange(seq_len).astype(F32)[:, None] * inv_freq[None, :]
    cos, sin = jnp.cos(angles), jnp.sin(angles)
    blank = jnp.zeros((seq_len, 128 - rope_dim), F32)
    return jnp.concatenate([cos, cos, blank], axis=1), jnp.concatenate([-sin, sin, blank], axis=1)


def clip_kernel(top, qb, kvb, y, new_qb, new_kvb, new_y):
    pair = pl.program_id(0)
    g0 = CLIP_TAU / jnp.maximum(CLIP_TAU, top[pl.ds(pair * 2, 1), :])
    g1 = CLIP_TAU / jnp.maximum(CLIP_TAU, top[pl.ds(pair * 2 + 1, 1), :])
    s0, s1 = jnp.sqrt(g0), jnp.sqrt(g1)
    low = lax.broadcasted_iota(jnp.int32, (1, 128), 1) < 64
    for j, gain in enumerate((s0, jnp.where(low, g0, s1), jnp.where(low, s1, g1))):
        cols = slice(j * 128, (j + 1) * 128)
        new_qb[:, cols] = (qb[:, cols].astype(F32) * gain).astype(BF16)
    for j, gain in ((0, s0), (2, s1)):
        cols = slice(j * 128, (j + 1) * 128)
        new_kvb[:, cols] = (kvb[:, cols].astype(F32) * gain).astype(BF16)
        cols = slice((j + 1) * 128, (j + 2) * 128)
        new_kvb[:, cols] = kvb[:, cols]
    new_y[...] = y[...]


def dot(a, b):
    return jnp.dot(a, b, preferred_element_type=F32)


def dot_t(a, b):
    return lax.dot_general(a, b, (((1,), (1,)), ((), ())), preferred_element_type=F32)


def kernel(dims, x_hbm, gin, gq, gkv, cos, sin, wqa_hbm, wkva_hbm, wqb_hbm, wkvb_hbm, wout_hbm,
           y_hbm, gall, gmine,
           xn, accq, acck, cq, ckv, krot, obuf, wqa, wkva, wqb, wkvb, wout,
           pbuf, r1, r2, r3, tbuf, xt, yt, smax, srecv,
           x_sem, a_sem, b_sem, o_sem, xt_sem, yt_sem,
           p_send, r1_recv, a_send, r2_recv, t_send, r3_recv, st_send, st_recv, g_send, g_recv):
    num_seqs, seq_len, model_dim, scale, rope_dim = dims
    q_rank = cq.shape[1]
    kv_rank = ckv.shape[1]
    tiles = model_dim // TILE
    units = model_dim // DEPTH
    pairs = wqb_hbm.shape[1] // 384
    halves = seq_len // ROWS
    chunks = num_seqs * halves
    total = chunks * tiles
    z = lax.axis_index("tp")
    dp = lax.axis_index("dp")
    is_mid = jnp.logical_or(z == 1, z == 2)
    is_end = jnp.logical_or(z == 0, z == 3)
    near = z + 1 - 2 * (z % 2)
    across = 3 - z
    dp_peer = [dp + 1 - 2 * (dp % 2), dp + 2 - 4 * ((dp // 2) % 2), dp + 4 - 8 * (dp // 4)]
    tp_peer = [(z + d) % 4 for d in (1, 2, 3)]

    barrier = pltpu.get_barrier_semaphore()
    for peer in dp_peer:
        pl.semaphore_signal(barrier, inc=1, device_id={"dp": peer}, device_id_type=MESH)
    for peer in tp_peer:
        pl.semaphore_signal(barrier, inc=1, device_id={"tp": peer}, device_id_type=MESH)
    pl.semaphore_wait(barrier, 6)

    def rows_of(c):
        return pl.ds(pl.multiple_of((c % halves) * ROWS, ROWS), ROWS)

    def x_copy(c):
        return pltpu.make_async_copy(x_hbm.at[c // halves, rows_of(c)], xn, x_sem)

    def a_copies(u):
        slot = u % 2
        rows = pl.ds(pl.multiple_of(u * DEPTH, DEPTH), DEPTH)
        return (pltpu.make_async_copy(wqa_hbm.at[rows], wqa.at[slot], a_sem.at[0, slot]),
                pltpu.make_async_copy(wkva_hbm.at[:, rows], wkva.at[slot], a_sem.at[1, slot]))

    def b_copies(hp):
        slot = hp % 2
        return (pltpu.make_async_copy(wqb_hbm.at[:, pl.ds(pl.multiple_of(hp * 384, 384), 384)], wqb.at[slot], b_sem.at[0, slot]),
                pltpu.make_async_copy(wkvb_hbm.at[:, pl.ds(pl.multiple_of(hp * 512, 512), 512)], wkvb.at[slot], b_sem.at[1, slot]))

    def cols_of(k):
        return pl.ds(pl.multiple_of((k % tiles) * TILE, TILE), TILE)

    def o_copy(k):
        return pltpu.make_async_copy(wout_hbm.at[:, cols_of(k)], wout.at[k % 2], o_sem.at[k % 2])

    def xt_copy(k):
        return pltpu.make_async_copy(x_hbm.at[k // (tiles * halves), rows_of(k // tiles), cols_of(k)], xt, xt_sem)

    def yt_copy(k):
        return pltpu.make_async_copy(yt.at[k % 2], y_hbm.at[k // (tiles * halves), rows_of(k // tiles), cols_of(k)], yt_sem.at[k % 2])

    def p_copy(k):
        return pltpu.make_async_remote_copy(
            src_ref=pbuf.at[k % SLOTS_P], dst_ref=r1.at[k % SLOTS_1], send_sem=p_send.at[k % SLOTS_P],
            recv_sem=r1_recv.at[k % SLOTS_1], device_id={"tp": near}, device_id_type=MESH)

    def a_copy(k):
        return pltpu.make_async_remote_copy(
            src_ref=pbuf.at[k % SLOTS_P], dst_ref=r2.at[k % SLOTS_2], send_sem=a_send.at[k % SLOTS_P],
            recv_sem=r2_recv.at[k % SLOTS_2], device_id={"tp": across}, device_id_type=MESH)

    def t_copy(k):
        return pltpu.make_async_remote_copy(
            src_ref=tbuf.at[k % SLOTS_T], dst_ref=r3.at[k % SLOTS_3], send_sem=t_send.at[k % SLOTS_T],
            recv_sem=r3_recv.at[k % SLOTS_3], device_id={"tp": near}, device_id_type=MESH)

    def st_copy(r):
        return pltpu.make_async_remote_copy(
            src_ref=smax, dst_ref=srecv.at[r], send_sem=st_send.at[r],
            recv_sem=st_recv.at[r], device_id={"dp": dp_peer[r]}, device_id_type=MESH)

    def g_copy(d):
        return pltpu.make_async_remote_copy(
            src_ref=smax, dst_ref=gall.at[z], send_sem=g_send.at[d],
            recv_sem=g_recv.at[d], device_id={"tp": tp_peer[d]}, device_id_type=MESH)

    def normalize():
        def block(i, carry):
            rows = pl.ds(pl.multiple_of(i * 16, 16), 16)
            v = xn[rows, :].astype(F32)
            inv = lax.rsqrt(jnp.mean(v * v, axis=-1, keepdims=True) + NORM_EPS)
            xn[rows, :] = (v * inv * gin[...]).astype(BF16)
            return carry
        lax.fori_loop(0, ROWS // 16, block, 0)

    def a_step(u):
        for c in a_copies(u):
            c.wait()

        @pl.when(u + 1 < units)
        def _():
            for c in a_copies(u + 1):
                c.start()

        slot = u % 2
        cols = pl.ds(pl.multiple_of(u * DEPTH, DEPTH), DEPTH)
        piece = xn[:, cols]
        width = 512

        @pl.when(u == 0)
        def _():
            for j in range(q_rank // width):
                accq[:, j * width:(j + 1) * width] = dot(piece, wqa[slot, :, j * width:(j + 1) * width])
            acck[...] = dot_t(piece, wkva[slot])

        @pl.when(u > 0)
        def _():
            for j in range(q_rank // width):
                accq[:, j * width:(j + 1) * width] += dot(piece, wqa[slot, :, j * width:(j + 1) * width])
            acck[...] += dot_t(piece, wkva[slot])

    def rope(v, c, s):
        half = rope_dim // 2
        lane = lax.broadcasted_iota(jnp.int32, v.shape, 1)
        swap = jnp.where(lane < half, pltpu.roll(v, 128 - half, 1), pltpu.roll(v, half, 1))
        return v * c + swap * s

    def finish_latents(half):
        def block(i, carry):
            rows = pl.ds(pl.multiple_of(i * 64, 64), 64)
            keys = pl.ds(pl.multiple_of(half * ROWS + i * 64, 64), 64)
            v = accq[rows, :]
            inv = lax.rsqrt(jnp.mean(v * v, axis=-1, keepdims=True) + NORM_EPS)
            cq[rows, :] = (v * inv * gq[...]).astype(BF16)
            w = acck[rows, :kv_rank]
            inv = lax.rsqrt(jnp.mean(w * w, axis=-1, keepdims=True) + NORM_EPS)
            ckv[keys, :] = (w * inv * gkv[...]).astype(BF16)
            kr = jnp.concatenate([acck[rows, kv_rank:], jnp.zeros((64, 128 - rope_dim), F32)], axis=1)
            krot[keys, :] = rope(kr, cos[keys, :], sin[keys, :]).astype(BF16)
            return carry
        lax.fori_loop(0, ROWS // 64, block, 0)

    def b_step(hp, oslot, half):
        for c in b_copies(hp):
            c.wait()

        @pl.when(hp + 1 < pairs)
        def _():
            for c in b_copies(hp + 1):
                c.start()

        slot = hp % 2
        for h in range(halves):
            @pl.when(half == h)
            def _(h=h):
                width = (h + 1) * ROWS
                mine = slice(h * ROWS, width)
                qf = dot(cq[...], wqb[slot])
                kv = dot(ckv[:width, :], wkvb[slot]).astype(BF16)
                qs = pltpu.roll(qf, 192, 1)
                for head, q2 in ((0, qf), (1, qs)):
                    q_rot = rope(q2[:, 128:256], cos[mine, :], sin[mine, :])
                    qcat = jnp.concatenate([q2[:, :128].astype(BF16), q_rot.astype(BF16)], axis=1)
                    kcat = jnp.concatenate([kv[:, head * 256:head * 256 + 128], krot[:width, :]], axis=1)
                    l = dot_t(qcat, kcat) * scale
                    row = lax.broadcasted_iota(jnp.int32, l.shape, 0) + h * ROWS
                    col = lax.broadcasted_iota(jnp.int32, l.shape, 1)
                    l = jnp.where(col <= row, l, -jnp.inf)
                    m = jnp.max(l, axis=-1, keepdims=True)
                    e = jnp.exp(l - m)
                    p = (e * (1.0 / jnp.sum(e, axis=-1, keepdims=True))).astype(BF16)
                    o = dot(p, kv[:, head * 256 + 128:head * 256 + 256]).astype(BF16)
                    obuf[oslot, :, pl.ds(pl.multiple_of(hp * 256 + head * 128, 128), 128)] = o
                    best = jnp.max(m, axis=0, keepdims=True)
                    r = pl.ds(hp * 2 + head, 1)
                    smax[r, :] = jnp.maximum(smax[r, :], jnp.broadcast_to(best, (1, 128)))

    def finish_tile(k, value):
        xt_copy(k).wait()

        @pl.when(k >= 2)
        def _():
            yt_copy(k - 2).wait()

        yt[k % 2] = (xt[...].astype(F32) + value).astype(BF16)
        yt_copy(k).start()

    smax[...] = jnp.full(smax.shape, -jnp.inf, F32)

    def tick(i):
        chunk = i // tiles
        t = i % tiles
        tau = i - tiles

        done_tile = jnp.where(is_mid, tau - LAG_MID, tau - LAG_END)

        @pl.when(jnp.logical_and(done_tile >= 0, done_tile < total))
        def _():
            xt_copy(done_tile).start()

        @pl.when(i == 0)
        def _():
            o_copy(0).start()

        @pl.when(jnp.logical_and(is_end, jnp.logical_and(tau >= SLOTS_P, tau < total + SLOTS_P)))
        def _():
            p_copy(tau - SLOTS_P).wait_send()

        @pl.when(jnp.logical_and(tau >= 0, tau < total))
        def _():
            o_copy(tau).wait()

            @pl.when(tau + 1 < total)
            def _():
                o_copy(tau + 1).start()

            pbuf[tau % SLOTS_P] = dot(obuf[(tau // tiles) % 2], wout[tau % 2])

            @pl.when(is_end)
            def _():
                p_copy(tau).start()

        @pl.when(jnp.logical_and(is_mid, jnp.logical_and(tau >= LAG_PAIR, tau < total + LAG_PAIR)))
        def _():
            k = tau - LAG_PAIR
            p_copy(k).wait_recv()
            pbuf[k % SLOTS_P] = pbuf[k % SLOTS_P] + r1[k % SLOTS_1]
            a_copy(k).start()

        @pl.when(jnp.logical_and(is_mid, jnp.logical_and(tau >= LAG_MID, tau < total + LAG_MID)))
        def _():
            k = tau - LAG_MID
            a_copy(k).wait()

            @pl.when(k >= SLOTS_T)
            def _():
                t_copy(k - SLOTS_T).wait_send()

            value = pbuf[k % SLOTS_P] + r2[k % SLOTS_2]
            tbuf[k % SLOTS_T] = value
            t_copy(k).start()
            finish_tile(k, value)

        @pl.when(jnp.logical_and(is_end, jnp.logical_and(tau >= LAG_END, tau < total + LAG_END)))
        def _():
            k = tau - LAG_END
            t_copy(k).wait_recv()
            finish_tile(k, r3[k % SLOTS_3])

        @pl.when(chunk < chunks)
        def _():
            half = chunk % halves

            @pl.when(t == 0)
            def _():
                x_copy(chunk).start()
                for c in a_copies(0):
                    c.start()
                for c in b_copies(0):
                    c.start()
                x_copy(chunk).wait()
                normalize()

            @pl.when(t < A_TICKS)
            def _():
                def step(j, carry):
                    a_step(t * (units // A_TICKS) + j)
                    return carry
                lax.fori_loop(0, units // A_TICKS, step, 0)

            @pl.when(t == A_TICKS - 1)
            def _():
                finish_latents(half)

            @pl.when(t >= A_TICKS)
            def _():
                def step(j, carry):
                    b_step((t - A_TICKS) * (pairs // (tiles - A_TICKS)) + j, chunk % 2, half)
                    return carry
                lax.fori_loop(0, pairs // (tiles - A_TICKS), step, 0)

    def stats_round(i):
        first = total
        for r in range(4):
            @pl.when(i == first + r)
            def _(r=r):
                if r > 0:
                    st_copy(r - 1).wait()
                    smax[...] = jnp.maximum(smax[...], srecv[r - 1])
                if r < 3:
                    st_copy(r).start()
                else:
                    gmine[...] = smax[...]
                    gall[z] = smax[...]
                    for d in range(3):
                        g_copy(d).start()

        @pl.when(i == first + 6)
        def _():
            for d in range(3):
                g_copy(d).wait()

    def whole_tick(i, carry):
        tick(i)
        stats_round(i)
        return carry

    lax.fori_loop(0, tiles + total + 7, whole_tick, 0)

    @pl.when(is_mid)
    def _():
        for k in range(total - SLOTS_T, total):
            t_copy(k).wait_send()
    for k in range(total - 2, total):
        yt_copy(k).wait()


def solution(mesh):
    def device_step(hidden, gain_in, gain_q, gain_kv, w_qa, w_kva, w_qb, w_kvb, w_out):
        num_seqs, seq_len, model_dim = hidden.shape
        q_rank, kv_rank = gain_q.shape[0], gain_kv.shape[0]
        rope_dim = w_kva.shape[1] - kv_rank
        num_heads = (w_qb.shape[1] - w_kvb.shape[1] + w_out.shape[0]) // rope_dim
        value_dim = w_out.shape[0] // num_heads
        nope_dim = w_kvb.shape[1] // num_heads - value_dim
        scale = (nope_dim + rope_dim) ** -0.5 * MSCALE_SQ
        cos, sin = rope_tables(seq_len, rope_dim)
        any_spec = pl.BlockSpec(memory_space=pl.ANY)
        vmem = pl.BlockSpec(memory_space=pltpu.VMEM)
        dma = pltpu.SemaphoreType.DMA
        block = (ROWS, TILE)
        y, gall, gmine = pl.pallas_call(
            lambda *refs: kernel((num_seqs, seq_len, model_dim, scale, rope_dim), *refs),
            out_shape=(jax.ShapeDtypeStruct(hidden.shape, BF16), jax.ShapeDtypeStruct((4, num_heads, 128), F32), jax.ShapeDtypeStruct((num_heads, 128), F32)),
            in_specs=[any_spec] + [vmem] * 5 + [any_spec] * 5,
            out_specs=(any_spec, vmem, vmem),
            scratch_shapes=[
                pltpu.VMEM((ROWS, model_dim), BF16),
                pltpu.VMEM((ROWS, q_rank), F32),
                pltpu.VMEM((ROWS, w_kva.shape[1]), F32),
                pltpu.VMEM((ROWS, q_rank), BF16),
                pltpu.VMEM((seq_len, kv_rank), BF16),
                pltpu.VMEM((seq_len, 128), BF16),
                pltpu.VMEM((2, ROWS, w_out.shape[0]), BF16),
                pltpu.VMEM((2, DEPTH, q_rank), BF16),
                pltpu.VMEM((2, w_kva.shape[1], DEPTH), BF16),
                pltpu.VMEM((2, q_rank, 384), BF16),
                pltpu.VMEM((2, kv_rank, 512), BF16),
                pltpu.VMEM((2, w_out.shape[0], TILE), BF16),
                pltpu.VMEM((SLOTS_P,) + block, F32),
                pltpu.VMEM((SLOTS_1,) + block, F32),
                pltpu.VMEM((SLOTS_2,) + block, F32),
                pltpu.VMEM((SLOTS_3,) + block, F32),
                pltpu.VMEM((SLOTS_T,) + block, F32),
                pltpu.VMEM(block, BF16),
                pltpu.VMEM((2,) + block, BF16),
                pltpu.VMEM((num_heads, 128), F32),
                pltpu.VMEM((3, num_heads, 128), F32),
                dma, dma((2, 2)), dma((2, 2)), dma((2,)), dma, dma((2,)),
                dma((SLOTS_P,)), dma((SLOTS_1,)), dma((SLOTS_P,)), dma((SLOTS_2,)), dma((SLOTS_T,)), dma((SLOTS_3,)),
                dma((3,)), dma((3,)), dma((3,)), dma((3,)),
            ],
            compiler_params=pltpu.CompilerParams(collective_id=0, has_side_effects=True, vmem_limit_bytes=66 * 1000 * 1000),
            name="latent_attention",
        )(hidden, gain_in[None], gain_q[None], gain_kv[None], cos, sin, w_qa, w_kva.T, w_qb, w_kvb, w_out)
        pairs = num_heads // 2
        y = y.reshape(num_seqs * seq_len, model_dim)
        share = y.shape[0] // pairs
        qb_block = pl.BlockSpec((q_rank, 384), lambda i: (0, i))
        kvb_block = pl.BlockSpec((kv_rank, 512), lambda i: (0, i))
        y_block = pl.BlockSpec((share, model_dim), lambda i: (i, 0))
        new_qb, new_kvb, y = pl.pallas_call(
            clip_kernel,
            grid=(pairs,),
            out_shape=(jax.ShapeDtypeStruct(w_qb.shape, BF16), jax.ShapeDtypeStruct(w_kvb.shape, BF16), jax.ShapeDtypeStruct(y.shape, BF16)),
            in_specs=[pl.BlockSpec((num_heads, 128), lambda i: (0, 0)), qb_block, kvb_block, y_block],
            out_specs=(qb_block, kvb_block, y_block),
            compiler_params=pltpu.CompilerParams(vmem_limit_bytes=32 * 1024 * 1024),
            name="clip_weights",
        )(gmine, w_qb, w_kvb, y)
        return y.reshape(hidden.shape), gall[:, :, 0].reshape(-1), new_qb, new_kvb

    weight_spec = P(None, 'tp')
    return jax.shard_map(device_step, mesh=mesh, in_specs=(P('dp', None, None), P(), P(), P(), P(), P(), weight_spec, weight_spec, P('tp', None)), out_specs=(P('dp', None, None), P(), weight_spec, weight_spec), check_vma=False)
```
